128 devices in a mesh: grp: 4 (over y), dom: 32 (over z, x, core).
Axes of the slice: x: 4, y: 4, z: 4, core: 2. Of those that a mesh axis runs over, the one named last changes fastest.
Arguments:
- table: float32 [524288, 256], P(('grp', 'dom')), may hold values from -6 to 6
- accum: float32 [524288], P(('grp', 'dom')), may hold values from 1e-07 to 0.0001
- w_self1: bfloat16 [256, 1024], replicated, may hold values from -0.375 to 0.375
- w_nbr1: bfloat16 [256, 1024], replicated, may hold values from -0.375 to 0.375
- w_self2: bfloat16 [1024, 1024], replicated, may hold values from -0.1875 to 0.1875
- w_nbr2: bfloat16 [1024, 1024], replicated, may hold values from -0.1875 to 0.1875
- fetch_owner: int32 [131072, 1], P(('grp', 'dom')), may hold values from 0 to 127; in each aligned block of 1024 rows (0 to 1023, 1024 to 2047, ...) at most 16 rows name the same one
- fetch_row: int32 [131072], P(('grp', 'dom')), may hold values from 0 to 4095
- self_slot: int32 [131072], P(('grp', 'dom')), may hold values from 0 to 1023
- nbr_one: int32 [131072, 8], P(('grp', 'dom')), may hold values from 0 to 1023
- nbr_two: int32 [131072, 8], P(('grp', 'dom')), may hold values from 0 to 1151
- cotangent: float32 [131072, 1024], P(('grp', 'dom')), may hold values from -0.06 to 0.06
Outputs:
- embedded: bfloat16 [131072, 1024], P(('grp', 'dom'))
- new_table: float32 [524288, 256], P(('grp', 'dom'))
- new_accum: float32 [524288], P(('grp', 'dom'))
- grad_self1: bfloat16 [256, 1024], replicated
- grad_nbr1: bfloat16 [256, 1024], replicated
- grad_self2: bfloat16 [1024, 1024], replicated
- grad_nbr2: bfloat16 [1024, 1024], replicated
The draws below stay inside these ranges and needn't reach their ends.
Inputs may be any that keep to these rules, and one draw needn't show every extreme that they name: `fetch_owner`: among the 1024 requests of one partition at most 16 name the same owner, and in some partition one owner is named exactly 16 times.
All inputs are finite; a program needn't handle non-finite values.
Results may differ from the reference program's by a relative error of at most 0.0045.
The reference program's roundings to bfloat16 on the way count: a program that leaves them out, or rounds other values in their place, can miss the bound.
Values may be sent and summed in bfloat16 or wider, within the bound.
No kernel may reach another device: no remote copies, remote signals or barrier semaphores. Data moves between devices by JAX's collectives and lax.ppermute only.
A program may use at most 128 MiB of HBM per device.

```python
import math
import jax
import jax.numpy as jnp
import numpy as np
from jax import lax

EMB = 256
HID = 1024
FANOUT = 8
BORDER = 64
FETCH = 1024
NODES = 1024
ROWS_DEV = 4096
CAP = 16
ROWS = 524288
FETCH_ALL = 131072
TOKENS = 131072
N_GRP = 4
N_DOM = 32
DEVICES = 128


def plant(result, stream_key, low, top_value):
    longest = result.shape.index(max(result.shape))
    spots = []
    for shift in (0, 1):
        where = [jax.random.randint(jax.random.fold_in(stream_key, axis), (), 0, length) for axis, length in enumerate(result.shape)]
        where[longest] = (where[longest] + shift) % result.shape[longest]
        spots.append(tuple(where))
    return result.at[spots[0]].set(low).at[spots[1]].set(top_value)


def block_levels(stream_key, shape, pieces, least, top_value):
    level = 1.0
    for axis_at, blocks in pieces:
        steps = jax.random.uniform(jax.random.fold_in(jax.random.fold_in(stream_key, 6), axis_at), (blocks,), jnp.float32, least / len(pieces), top_value / len(pieces))
        level = level * jnp.repeat(jnp.exp(steps), shape[axis_at] // blocks).reshape((-1,) + (1,) * (len(shape) - 1 - axis_at))
    return level


def routed_block(stream_key, own, number, rows, count, top, most, slope):
    sequence = jax.random.permutation(stream_key, count)
    packed, ordinary = shares(count, rows * top, most, slope, True), shares(count, rows * top, most, slope, False)
    places = jnp.arange(count)

    def named(tallies, offset_by):
        used = int((tallies > 0).sum())
        fixed = max(1, used // 4)
        shifted = fixed + (places - fixed + offset_by * (used - fixed)) % max(1, count - fixed)
        return jnp.zeros((count,), jnp.int32).at[sequence[jnp.where(places < fixed, places, shifted)]].set(jnp.asarray(tallies, jnp.int32))

    tallies = jnp.where(number % 4 == 0, named(packed, number // 4), named(ordinary, number - number // 4 - 1))
    mixed = jax.random.permutation(jax.random.fold_in(own, 3), count)
    giver, taker = mixed[0:count // 2 * 2:2], mixed[1:count // 2 * 2:2]
    room = jnp.minimum(tallies[giver] - 1, most - tallies[taker]) // 2
    room = jnp.where((giver == sequence[0]) | (taker == sequence[0]) | (tallies[taker] == 0), 0, jnp.maximum(room, 0))
    shifted = jax.random.randint(jax.random.fold_in(own, 4), (count // 2,), 0, 1 << 20) % (room + 1)
    tallies = tallies.at[giver].add(-shifted).at[taker].add(shifted)
    members = jnp.searchsorted(jnp.cumsum(tallies), jnp.arange(rows * top), side="right").astype(jnp.int32)
    grid = members.reshape(top, rows).T
    grid = grid[jax.random.permutation(jax.random.fold_in(own, 1), rows)]
    offset_by = jax.random.randint(jax.random.fold_in(own, 2), (rows, 1), 0, top)
    return jnp.take_along_axis(grid, (jnp.arange(top)[None, :] + offset_by) % top, axis=1)


def shares(count, total, most, lean, full):
    weights = [(1 << 20) // math.isqrt(standing ** lean) + 1 for standing in range(1, count + 1)]
    largest = most if full else min(most, max(-(-total // count), total * weights[0] // sum(weights)))
    least = 1 if total - largest >= count - 1 else 0
    given, surplus = [largest] + [least] * (count - 1), total - largest - least * (count - 1)
    while surplus > 0:
        movable = [i for i in range(1, count) if given[i] < largest] or [i for i in range(1, count) if given[i] < most]
        pool, left = sum([weights[i] for i in movable]), surplus
        for i in movable:
            more = min(most - given[i], max(1, left * weights[i] // pool), surplus)
            given[i] = given[i] + more
            surplus = surplus - more
    return np.array(given)


def scatter_about(own_key, extent, scale, most, split=(), held_as=jnp.bfloat16):
    entries = scale * jax.random.normal(own_key, extent, jnp.float32)
    if split:
        entries = entries * block_levels(own_key, extent, split, -0.22, 0.18)
    return jnp.clip(entries, -most, most).astype(held_as)


def setup_inputs(seed: int = 0) -> dict:
    key_list = jax.random.split(jax.random.key(seed), 13)
    table = scatter_about(key_list[0], (ROWS, EMB), 1.0, 6.0, ((0, 128),), jnp.float32)
    accum = jnp.clip(jnp.exp(math.log(0.0001) - 6.9077552 * jax.random.uniform(key_list[1], (ROWS,), jnp.float32) ** block_levels(key_list[1], (ROWS,), ((0, 128),), -0.2, 0.2)), 1.0000000116860974e-07, 0.0001)
    w_self1 = scatter_about(key_list[2], (EMB, HID), EMB ** -0.5, 0.375)
    w_nbr1 = scatter_about(key_list[3], (EMB, HID), EMB ** -0.5, 0.375)
    w_self2 = scatter_about(key_list[4], (HID, HID), HID ** -0.5, 0.1875)
    w_nbr2 = scatter_about(key_list[5], (HID, HID), HID ** -0.5, 0.1875)
    fetch_owner_keys = jax.random.split(jax.random.fold_in(key_list[6], 1), FETCH_ALL // FETCH)
    fetch_owner_turns = jax.random.permutation(jax.random.fold_in(key_list[6], 3), FETCH_ALL // FETCH)
    fetch_owner = jax.vmap(lambda own, number: routed_block(jax.random.fold_in(key_list[6], 2), own, number, FETCH, DEVICES, 1, CAP, 2))(fetch_owner_keys, fetch_owner_turns).reshape((FETCH_ALL, 1))
    fetch_row = plant(jax.random.randint(key_list[7], (FETCH_ALL,), 0, ROWS_DEV), jax.random.fold_in(key_list[7], 1), 0, ROWS_DEV - 1).astype(jnp.int32)
    self_slot = plant(jax.random.randint(key_list[8], (TOKENS,), 0, FETCH), jax.random.fold_in(key_list[8], 1), 0, FETCH - 1).astype(jnp.int32)
    nbr_one = plant(jax.random.randint(key_list[9], (TOKENS, FANOUT), 0, FETCH), jax.random.fold_in(key_list[9], 1), 0, FETCH - 1).astype(jnp.int32)
    nbr_two = plant(jax.random.randint(key_list[10], (TOKENS, FANOUT), 0, NODES + 2 * BORDER), jax.random.fold_in(key_list[10], 1), 0, (NODES + 2 * BORDER) - 1).astype(jnp.int32)
    cotangent = scatter_about(key_list[11], (TOKENS, HID), 0.01, 0.06, ((0, 128),), jnp.float32)
    return {"table": table, "accum": accum, "w_self1": w_self1, "w_nbr1": w_nbr1, "w_self2": w_self2, "w_nbr2": w_nbr2, "fetch_owner": fetch_owner, "fetch_row": fetch_row, "self_slot": self_slot, "nbr_one": nbr_one, "nbr_two": nbr_two, "cotangent": cotangent}


epsilon = 1e-06
learning_rate = 0.1

def swish_slope(values):
    logistic = jax.nn.sigmoid(values)
    return logistic + values * logistic * (1.0 - logistic)

def counts(neighbours, widths):
    hits = (neighbours[:, :, None] == jnp.arange(widths, dtype=jnp.int32)[None, None, :]).astype(jnp.float32)
    return lax.optimization_barrier(jnp.sum(hits, axis=1)).astype(jnp.bfloat16)

def contract_rows(left, right):
    return lax.dot_general(left, right, (((0,), (0,)), ((), ())), preferred_element_type=jnp.float32)

def contract_cols(left, right):
    return lax.dot_general(left, right, (((1,), (1,)), ((), ())), preferred_element_type=jnp.float32)

def forward_one(fetched, slot_index, neighbours, w_self1, w_nbr1):
    fanout = neighbours.shape[1]
    self_rows = fetched[slot_index]
    adjacency_one = counts(neighbours, fetched.shape[0])
    pooled_one = (jnp.dot(adjacency_one, fetched, preferred_element_type=jnp.float32) / fanout).astype(jnp.bfloat16)
    before_one = jnp.dot(self_rows, w_self1, preferred_element_type=jnp.float32) + jnp.dot(pooled_one, w_nbr1, preferred_element_type=jnp.float32)
    return (self_rows, adjacency_one, pooled_one, before_one)

def forward_two(hidden_one, bordered, neighbours, w_self2, w_nbr2):
    fanout = neighbours.shape[1]
    adjacency_two = counts(neighbours, bordered.shape[0])
    pooled_two = (jnp.dot(adjacency_two, bordered, preferred_element_type=jnp.float32) / fanout).astype(jnp.bfloat16)
    before_two = jnp.dot(hidden_one, w_self2, preferred_element_type=jnp.float32) + jnp.dot(pooled_two, w_nbr2, preferred_element_type=jnp.float32)
    lifted = jax.nn.silu(before_two)
    scale = lax.rsqrt(lax.optimization_barrier(jnp.mean(lifted * lifted, axis=1, keepdims=True)) + epsilon)
    return (adjacency_two, pooled_two, before_two, lifted * scale, scale)

def backward_two(upstream, hidden_one, adjacency_two, pooled_two, before_two, normed, scale, w_self2, w_nbr2):
    fanout_inv = 1.0 / FANOUT
    grad_lifted = scale * (upstream - normed * lax.optimization_barrier(jnp.mean(upstream * normed, axis=1, keepdims=True)))
    grad_before = (grad_lifted * swish_slope(before_two)).astype(jnp.bfloat16)
    g_self2 = contract_rows(hidden_one, grad_before)
    g_nbr2 = contract_rows(pooled_two, grad_before)
    grad_hidden = contract_cols(grad_before, w_self2)
    grad_pooled = contract_cols(grad_before, w_nbr2).astype(jnp.bfloat16)
    grad_bordered = contract_rows(adjacency_two, grad_pooled) * fanout_inv
    return (g_self2, g_nbr2, grad_hidden, grad_bordered)

def backward_one(grad_hidden, before_one, self_rows, adjacency_one, pooled_one, slot_index, w_self1, w_nbr1):
    fanout_inv = 1.0 / FANOUT
    grad_before = (grad_hidden * swish_slope(before_one)).astype(jnp.bfloat16)
    g_self1 = contract_rows(self_rows, grad_before)
    g_nbr1 = contract_rows(pooled_one, grad_before)
    grad_self_rows = contract_cols(grad_before, w_self1)
    grad_pooled = contract_cols(grad_before, w_nbr1).astype(jnp.bfloat16)
    grad_fetched = jax.ops.segment_sum(grad_self_rows, slot_index, num_segments=adjacency_one.shape[1])
    grad_fetched = grad_fetched + contract_rows(adjacency_one, grad_pooled) * fanout_inv
    return (g_self1, g_nbr1, grad_fetched)

def reference(table, accum, w_self1, w_nbr1, w_self2, w_nbr2, fetch_owner, fetch_row, self_slot, nbr_one, nbr_two, cotangent):
    parts = N_GRP * N_DOM
    global_rows = (fetch_owner[:, 0] * ROWS_DEV + fetch_row).astype(jnp.int32)
    fetched = table[global_rows].astype(jnp.bfloat16).reshape(parts, FETCH, EMB)
    slots = self_slot.reshape(parts, NODES)
    first_lists = nbr_one.reshape(parts, NODES, FANOUT)
    second_lists = nbr_two.reshape(parts, NODES, FANOUT)
    upstream_all = cotangent.reshape(parts, NODES, HID)

    def hidden_of(inputs):
        rows, slot_index, lists = inputs
        outcome = forward_one(rows, slot_index, lists, w_self1, w_nbr1)
        return jax.nn.silu(outcome[3]).astype(jnp.bfloat16)
    hidden_one = lax.map(hidden_of, (fetched, slots, first_lists))
    bordered = jnp.concatenate([jnp.roll(hidden_one, 1, axis=0)[:, NODES - BORDER:], hidden_one, jnp.roll(hidden_one, -1, axis=0)[:, :BORDER]], axis=1)

    def second_step(carry, inputs):
        hidden, bordered_rows, lists, upstream = inputs
        adjacency_two, pooled_two, before_two, normed, scale = forward_two(hidden, bordered_rows, lists, w_self2, w_nbr2)
        g_self2, g_nbr2, grad_hidden, grad_bordered = backward_two(upstream, hidden, adjacency_two, pooled_two, before_two, normed, scale, w_self2, w_nbr2)
        middle = grad_hidden + grad_bordered[BORDER:BORDER + NODES]
        edges = jnp.concatenate([grad_bordered[:BORDER], grad_bordered[BORDER + NODES:]], axis=0)
        return ((carry[0] + g_self2, carry[1] + g_nbr2), (normed.astype(jnp.bfloat16), middle, edges))
    zero_hh = jnp.zeros((HID, HID), jnp.float32)
    (sum_self2, sum_nbr2), (embedded, middle, edges) = lax.scan(second_step, (zero_hh, zero_hh), (hidden_one, bordered, second_lists, upstream_all))
    from_before = jnp.roll(edges, 1, axis=0)[:, BORDER:]
    from_after = jnp.roll(edges, -1, axis=0)[:, :BORDER]
    grad_hidden_all = middle.at[:, :BORDER].add(from_before).at[:, NODES - BORDER:].add(from_after)

    def first_step(carry, inputs):
        rows, slot_index, lists, grad_hidden = inputs
        self_rows, adjacency_one, pooled_one, before_one = forward_one(rows, slot_index, lists, w_self1, w_nbr1)
        g_self1, g_nbr1, grad_fetched = backward_one(grad_hidden, before_one, self_rows, adjacency_one, pooled_one, slot_index, w_self1, w_nbr1)
        return ((carry[0] + g_self1, carry[1] + g_nbr1), grad_fetched)
    zero_eh = jnp.zeros((EMB, HID), jnp.float32)
    (sum_self1, sum_nbr1), grad_fetched = lax.scan(first_step, (zero_eh, zero_eh), (fetched, slots, first_lists, grad_hidden_all))
    row_grads = jax.ops.segment_sum(grad_fetched.reshape(-1, EMB), global_rows, num_segments=ROWS_DEV * N_GRP * N_DOM)
    new_accum = accum + lax.optimization_barrier(jnp.mean(row_grads * row_grads, axis=1))
    new_table = table - learning_rate * row_grads / (jnp.sqrt(new_accum)[:, None] + epsilon)
    return (embedded.reshape(-1, HID), new_table, new_accum, sum_self1.astype(jnp.bfloat16), sum_nbr1.astype(jnp.bfloat16), sum_self2.astype(jnp.bfloat16), sum_nbr2.astype(jnp.bfloat16))
```

```python
import jax
import jax.numpy as jnp
from jax import lax
from jax.experimental import pallas as pl
from jax.experimental.pallas import tpu as pltpu
from jax.sharding import PartitionSpec as P


BORDER = 64
AXES = ("grp", "dom")
epsilon = 1e-06
learning_rate = 0.1
BF = jnp.bfloat16
F32 = jnp.float32
I32 = jnp.int32
I16 = jnp.int16
MIB = 1024 * 1024


def iota(shape, dim):
    return lax.broadcasted_iota(I32, shape, dim)


def nn(a, b):
    return lax.dot_general(a, b, (((1,), (0,)), ((), ())), preferred_element_type=F32)


def nt(a, b):
    return lax.dot_general(a, b, (((1,), (1,)), ((), ())), preferred_element_type=F32)


def tn(a, b):
    return lax.dot_general(a, b, (((0,), (0,)), ((), ())), preferred_element_type=F32)


def hot(mask):
    return jnp.where(mask, 1.0, 0.0).astype(BF)


def hot_lanes(col, width):
    lanes = col.shape[1]
    index = iota(col.shape, 1).astype(I16)
    parts = []
    for at in range(0, width, lanes):
        hit = col == index + jnp.full(col.shape, at, I16)
        parts.append(jnp.where(hit, jnp.ones(col.shape, BF), jnp.zeros(col.shape, BF)))
    return jnp.concatenate(parts, axis=1)


def hot_rows(row, rows, first):
    shape = (rows, row.shape[1])
    index = iota(shape, 0).astype(I16)
    wanted = jnp.broadcast_to(row - first, shape).astype(I16)
    return jnp.where(index == wanted, jnp.ones(shape, BF), jnp.zeros(shape, BF))


def to_lanes(row):
    return jnp.broadcast_to(row, (128, row.shape[1])).T.astype(I16)


def logistic(v):
    return 1.0 / (1.0 + jnp.exp(-v))


def params(mib, *semantics):
    return pltpu.CompilerParams(
        dimension_semantics=semantics if semantics else None, vmem_limit_bytes=mib * MIB
    )


def in_hbm(x):
    return pltpu.with_memory_space_constraint(x, pltpu.HBM)


def cost(flops):
    return pl.CostEstimate(flops=flops, bytes_accessed=4 << 20, transcendentals=0)


def prep_kernel(owner_ref, row_ref, pos_ref, wanted_ref):
    count = owner_ref.shape[1]
    devices, cap = wanted_ref.shape
    owner = owner_ref[...]
    row = row_ref[...]
    owner_hot = hot(iota((devices, count), 0) == owner)
    earlier = hot(iota((count, count), 0) < iota((count, count), 1))
    before = nn(owner_hot, earlier)
    rank = jnp.sum(before * owner_hot.astype(F32), axis=0, keepdims=True).astype(I32)
    pos_ref[...] = owner * cap + rank
    at_rank = iota((cap, count), 0) == rank
    high = jnp.where(at_rank, (row >> 6).astype(F32), 0.0).astype(BF)
    low = jnp.where(at_rank, (row & 63).astype(F32), 0.0).astype(BF)
    wanted_ref[...] = (nt(owner_hot, high) * 64.0 + nt(owner_hot, low)).astype(I32)


def prep(owner, row, devices, cap):
    count = owner.shape[1]
    return pl.pallas_call(
        prep_kernel,
        out_shape=(
            jax.ShapeDtypeStruct((1, count), I32),
            jax.ShapeDtypeStruct((devices, cap), I32),
        ),
        compiler_params=params(8),
        name="prep",
    )(owner, row)


def counts_kernel(shift, width, nbr_ref, *out_refs):
    fanout, lanes = nbr_ref.shape
    base = 0
    lists = []
    for k in range(fanout):
        row = nbr_ref[k : k + 1, :]
        if shift:
            row = row - shift
            row = jnp.where(row < 0, row + width, row)
        lists.append(jnp.broadcast_to(row, (16, lanes)).astype(I16))
    index = iota((16, lanes), 0).astype(I16)
    unit = jnp.full((16, lanes), 1.0 / fanout, BF)
    none = jnp.zeros((16, lanes), BF)
    for adj_t_ref, adj_ref in zip(out_refs[::2], out_refs[1::2]):
        for first in range(0, adj_t_ref.shape[0], 128):
            rows = []
            for r in range(first, first + 128, 16):
                at = index + jnp.full((16, lanes), base + r, I16)
                acc = none
                for k in range(fanout):
                    acc = acc + jnp.where(lists[k] == at, unit, none)
                rows.append(acc)
            block = jnp.concatenate(rows, axis=0)
            adj_t_ref[first : first + 128, :] = block
            adj_ref[:, first : first + 128] = block.T
        base += adj_t_ref.shape[0]


def counts(nbr_t, widths, shift):
    fanout, nodes = nbr_t.shape
    block = 128
    specs, shapes = [], []
    for width in widths:
        specs += [
            pl.BlockSpec((width, block), lambda i: (0, i)),
            pl.BlockSpec((block, width), lambda i: (i, 0)),
        ]
        shapes += [pltpu.HBM((width, nodes), BF), pltpu.HBM((nodes, width), BF)]
    return pl.pallas_call(
        lambda *refs: counts_kernel(shift, sum(widths), *refs),
        grid=(nodes // block,),
        in_specs=[pl.BlockSpec((fanout, block), lambda i: (0, i))],
        out_specs=specs,
        out_shape=shapes,
        compiler_params=params(8, "arbitrary"),
        cost_estimate=cost(4 << 30),
    )(nbr_t)


def pick_kernel(inc_ref, table_ref, out_ref, col_ref, acc_ref, turn_ref):
    i = pl.program_id(0)
    peers, cap = inc_ref.shape
    rows, width = table_ref.shape

    @pl.when(i == 0)
    def _():
        for c in range(cap):
            col_ref[c * peers : (c + 1) * peers, :] = jnp.broadcast_to(
                inc_ref[:, c : c + 1], (peers, 128)
            ).astype(I16)

    def step(j, carry):
        first = pl.multiple_of(j * 256, 256)
        chunk = table_ref[pl.ds(first, 256), :].astype(BF)
        base = (jnp.zeros(col_ref.shape, I32) + (i * rows + first)).astype(I16)
        part = nn(hot_lanes(col_ref[...] - base, 256), chunk)
        fresh = jnp.logical_and(i == 0, j == 0)

        @pl.when(fresh)
        def _():
            acc_ref[...] = part

        @pl.when(jnp.logical_not(fresh))
        def _():
            acc_ref[...] += part

        return carry

    lax.fori_loop(0, rows // 256, step, 0)

    @pl.when(i == pl.num_programs(0) - 1)
    def _():
        for c in range(cap):
            for h in range(width // 128):
                turn_ref.at[h][pl.ds(c, peers, stride=cap), :] = acc_ref[
                    c * peers : (c + 1) * peers, h * 128 : (h + 1) * 128
                ]
        for h in range(width // 128):
            out_ref[:, h * 128 : (h + 1) * 128] = turn_ref[h].astype(BF)


def pick(incoming, table):
    devices, cap = incoming.shape
    rows, width = table.shape
    slots = devices * cap
    block = 1024
    return pl.pallas_call(
        pick_kernel,
        grid=(rows // block,),
        in_specs=[
            pl.BlockSpec((devices, cap), lambda i: (0, 0)),
            pl.BlockSpec((block, width), lambda i: (i, 0)),
        ],
        out_specs=pl.BlockSpec((slots, width), lambda i: (0, 0)),
        out_shape=pltpu.HBM((slots, width), BF),
        scratch_shapes=[
            pltpu.VMEM((slots, 128), I16),
            pltpu.VMEM((slots, width), F32),
            pltpu.VMEM((width // 128, slots, 128), F32),
        ],
        compiler_params=params(24, "arbitrary"),
        name="pick",
    )(incoming, in_hbm(table))


def layer_one_kernel(
    pos_ref, slot_ref, replies_ref, adj_ref, ws_ref, wn_ref,
    selfs_ref, pooled_ref, before_ref, hidden_ref, fetched_ref,
):
    i = pl.program_id(0)
    _, fetch = adj_ref.shape
    slots = replies_ref.shape[0]

    @pl.when(i == 0)
    def _():
        for at in range(0, fetch, 512):
            place = hot_lanes(to_lanes(pos_ref[:, at : at + 512]), slots)
            fetched_ref[at : at + 512, :] = nn(place, replies_ref[...]).astype(BF)

    @pl.when(i > 0)
    def _():
        self_hot = hot_lanes(to_lanes(slot_ref[...]), fetch)
        selfs = nn(self_hot, fetched_ref[...]).astype(BF)
        pooled = nn(adj_ref[...], fetched_ref[...]).astype(BF)
        selfs_ref[...] = selfs
        pooled_ref[...] = pooled
        before = nn(selfs, ws_ref[...]) + nn(pooled, wn_ref[...])
        before_ref[...] = before
        hidden_ref[...] = (before * logistic(before)).astype(BF)


def layer_one(pos, slot, replies, adj, w_self, w_nbr):
    nodes, fetch = adj.shape
    slots = replies.shape[0]
    emb, hid = w_self.shape
    block = 512
    late = lambda i: (jnp.maximum(i - 1, 0), 0)
    whole = lambda i: (0, 0)
    return pl.pallas_call(
        layer_one_kernel,
        grid=(1 + nodes // block,),
        in_specs=[
            pl.BlockSpec((1, fetch), whole),
            pl.BlockSpec((1, block), lambda i: (0, jnp.maximum(i - 1, 0))),
            pl.BlockSpec((slots, emb), whole),
            pl.BlockSpec((block, fetch), late),
            pl.BlockSpec((emb, hid), whole),
            pl.BlockSpec((emb, hid), whole),
        ],
        out_specs=[
            pl.BlockSpec((block, emb), late),
            pl.BlockSpec((block, emb), late),
            pl.BlockSpec((block, hid), late),
            pl.BlockSpec((block, hid), late),
        ],
        out_shape=(
            pltpu.HBM((nodes, emb), BF),
            pltpu.HBM((nodes, emb), BF),
            pltpu.HBM((nodes, hid), F32),
            jax.ShapeDtypeStruct((nodes, hid), BF),
        ),
        scratch_shapes=[pltpu.VMEM((fetch, emb), BF)],
        compiler_params=params(28, "arbitrary"),
        name="layer_one",
    )(pos, slot, in_hbm(replies), in_hbm(adj), in_hbm(w_self), in_hbm(w_nbr))


def layer_two_kernel(
    own_ref, pool_ref, edge_ref, edge_t_ref, after_ref, before_in_ref, wn_ref, up_ref,
    emb_ref, pooled_ref, grad_ref, gpool_ref, gedge_ref,
):
    i = pl.program_id(0)
    halo = jnp.concatenate([after_ref[...], before_in_ref[...]], axis=0)
    pooled = (pool_ref[...] + nn(edge_ref[...], halo)).astype(BF)
    pooled_ref[...] = pooled
    before = own_ref[...] + nn(pooled, wn_ref[...])
    gate = logistic(before)
    lifted = before * gate
    scale = lax.rsqrt(jnp.mean(lifted * lifted, axis=1, keepdims=True) + epsilon)
    normed = lifted * scale
    emb_ref[...] = normed.astype(BF)
    up = up_ref[...]
    grad_lifted = scale * (up - normed * jnp.mean(up * normed, axis=1, keepdims=True))
    grad = (grad_lifted * (gate + lifted * (1.0 - gate))).astype(BF)
    grad_ref[...] = grad
    gpool = nt(grad, wn_ref[...]).astype(BF)
    gpool_ref[...] = gpool
    part = nn(edge_t_ref[...], gpool)

    @pl.when(i == 0)
    def _():
        gedge_ref[...] = part

    @pl.when(i > 0)
    def _():
        gedge_ref[...] += part


def layer_two(own, pool, edge, edge_t, after, before, w_nbr, upstream):
    nodes, hid = own.shape
    block = 256
    rows = lambda i: (i, 0)
    whole = lambda i: (0, 0)
    return pl.pallas_call(
        layer_two_kernel,
        grid=(nodes // block,),
        in_specs=[
            pl.BlockSpec((block, hid), rows),
            pl.BlockSpec((block, hid), rows),
            pl.BlockSpec((block, 2 * BORDER), rows),
            pl.BlockSpec((2 * BORDER, block), lambda i: (0, i)),
            pl.BlockSpec((BORDER, hid), whole),
            pl.BlockSpec((BORDER, hid), whole),
            pl.BlockSpec((hid, hid), whole),
            pl.BlockSpec((block, hid), rows),
        ],
        out_specs=[
            pl.BlockSpec((block, hid), rows),
            pl.BlockSpec((block, hid), rows),
            pl.BlockSpec((block, hid), rows),
            pl.BlockSpec((block, hid), rows),
            pl.BlockSpec((2 * BORDER, hid), whole),
        ],
        out_shape=(
            jax.ShapeDtypeStruct((nodes, hid), BF),
            jax.ShapeDtypeStruct((nodes, hid), BF),
            jax.ShapeDtypeStruct((nodes, hid), BF),
            jax.ShapeDtypeStruct((nodes, hid), BF),
            jax.ShapeDtypeStruct((2 * BORDER, hid), F32),
        ),
        compiler_params=params(28, "arbitrary"),
        name="layer_two",
    )(own, pool, edge, edge_t, after, before, w_nbr, upstream)


def back_one_kernel(
    gh_ref, first_ref, last_ref, before_ref, slot_ref, adj_t_ref, ws_ref, wn_ref, pos_ref,
    grad_ref, out_ref, gh_scr, acc_ref,
):
    i = pl.program_id(0)
    last = pl.num_programs(0) - 1
    block = gh_ref.shape[0]
    fetch = acc_ref.shape[0]
    gh_scr[...] = gh_ref[...]

    @pl.when(i == 0)
    def _():
        gh_scr[0:BORDER, :] += first_ref[...]

    @pl.when(i == last)
    def _():
        gh_scr[block - BORDER : block, :] += last_ref[...]

    before = before_ref[...]
    gate = logistic(before)
    grad = (gh_scr[...] * (gate + before * gate * (1.0 - gate))).astype(BF)
    grad_ref[...] = grad
    gself = nt(grad, ws_ref[...])
    high = gself.astype(BF)
    low = (gself - high.astype(F32)).astype(BF)
    gpool = nt(grad, wn_ref[...]).astype(BF)
    self_t = hot_rows(slot_ref[...], fetch, 0)
    part = nn(self_t, high) + nn(self_t, low) + nn(adj_t_ref[...], gpool)

    @pl.when(i == 0)
    def _():
        acc_ref[...] = part

    @pl.when(i > 0)
    def _():
        acc_ref[...] += part

    @pl.when(i == last)
    def _():
        total = acc_ref[...].astype(BF)
        pos = pos_ref[...]
        slots = out_ref.shape[0]
        for at in range(0, slots, 256):
            place_t = hot_rows(pos, 256, at)
            out_ref[at : at + 256, :] = nn(place_t, total).astype(BF)


def back_one(gh, first, last, before, slot, adj_t, w_self, w_nbr, pos, slots):
    nodes, hid = gh.shape
    emb = w_self.shape[0]
    fetch = adj_t.shape[0]
    block = 256
    rows = lambda i: (i, 0)
    cols = lambda i: (0, i)
    whole = lambda i: (0, 0)
    return pl.pallas_call(
        back_one_kernel,
        grid=(nodes // block,),
        in_specs=[
            pl.BlockSpec((block, hid), rows),
            pl.BlockSpec((BORDER, hid), whole),
            pl.BlockSpec((BORDER, hid), whole),
            pl.BlockSpec((block, hid), rows),
            pl.BlockSpec((1, block), cols),
            pl.BlockSpec((fetch, block), cols),
            pl.BlockSpec((emb, hid), whole),
            pl.BlockSpec((emb, hid), whole),
            pl.BlockSpec((1, fetch), whole),
        ],
        out_specs=[
            pl.BlockSpec((block, hid), rows),
            pl.BlockSpec((slots, emb), whole),
        ],
        out_shape=(
            pltpu.HBM((nodes, hid), BF),
            pltpu.HBM((slots, emb), BF),
        ),
        scratch_shapes=[pltpu.VMEM((block, hid), F32), pltpu.VMEM((fetch, emb), F32)],
        compiler_params=params(24, "arbitrary"),
        name="back_one",
    )(gh, first, last, before, slot, adj_t, w_self, w_nbr, pos)


def update_kernel(
    inc_ref, got_ref, table_ref, accum_ref, new_table_ref, new_accum_ref, returned_ref
):
    i = pl.program_id(0)
    block, width = table_ref.shape
    slots = returned_ref.shape[0]
    peers = got_ref.shape[0]

    @pl.when(i == 0)
    def _():
        returned_ref[...] = got_ref[:, : slots // peers, :].reshape(slots, width)

    inc = inc_ref[...]
    step = 512
    grads = jnp.zeros((block, width), F32)
    for at in range(0, slots, step):
        rows_hot = hot_rows(inc[:, at : at + step], block, i * block)
        grads = grads + nn(rows_hot, returned_ref[at : at + step, :])
    square = jnp.mean(grads * grads, axis=1, keepdims=True)
    accum = accum_ref[0]
    new_accum_ref[0] = accum + jnp.broadcast_to(square, (block, 128)).T[0:1, :]
    total = jnp.broadcast_to(accum, (128, block)).T + square
    factor = learning_rate / (jnp.sqrt(total) + epsilon)
    for at in range(0, width, 128):
        new_table_ref[:, at : at + 128] = (
            table_ref[:, at : at + 128] - grads[:, at : at + 128] * factor
        )


def update(inc_row, got, table, accum):
    rows, width = table.shape
    slots = inc_row.shape[1]
    block = 512
    shaped = accum.reshape(rows // block, 1, block)
    new_table, new_accum = pl.pallas_call(
        update_kernel,
        grid=(rows // block,),
        in_specs=[
            pl.BlockSpec((1, slots), lambda i: (0, 0)),
            pl.BlockSpec(got.shape, lambda i: (0, 0, 0)),
            pl.BlockSpec((block, width), lambda i: (i, 0)),
            pl.BlockSpec((1, 1, block), lambda i: (i, 0, 0)),
        ],
        out_specs=[
            pl.BlockSpec((block, width), lambda i: (i, 0)),
            pl.BlockSpec((1, 1, block), lambda i: (i, 0, 0)),
        ],
        out_shape=(
            jax.ShapeDtypeStruct((rows, width), F32),
            jax.ShapeDtypeStruct(shaped.shape, F32),
        ),
        scratch_shapes=[pltpu.VMEM((slots, width), BF)],
        compiler_params=params(16, "arbitrary"),
        cost_estimate=cost(4 << 30),
        name="update",
    )(inc_row, in_hbm(got), in_hbm(table), shaped)
    return new_table, new_accum.reshape(rows)


def chip_sums(parts_ref, core):
    total = parts_ref[core].astype(F32)
    for at in range(core + 2, parts_ref.shape[0], 2):
        total = total + parts_ref[at].astype(F32)
    return total.astype(BF)


def two_sum_kernel(parts_ref, out_ref):
    for core in range(2):
        out_ref[core] = chip_sums(parts_ref, core)


def two_sum(parts):
    peers, rows, width = parts.shape
    lanes = 512
    return pl.pallas_call(
        two_sum_kernel,
        grid=(width // lanes,),
        in_specs=[pl.BlockSpec((peers, rows, lanes), lambda i: (0, 0, i))],
        out_specs=pl.BlockSpec((2, rows, lanes), lambda i: (0, 0, i)),
        out_shape=jax.ShapeDtypeStruct((2, rows, width), BF),
        compiler_params=params(8, "arbitrary"),
        cost_estimate=cost(1 << 30),
        name="two_sum",
    )(in_hbm(parts))


def spread_kernel(two_ref, got_ref, out_ref):
    i = pl.program_id(0)
    peers = out_ref.shape[0]
    last = pl.num_programs(0) - 1

    @pl.when(i < last)
    def _():
        for core in range(2):
            for at in range(core, peers, 2):
                out_ref[at] = two_ref[core]

    @pl.when(i == last)
    def _():
        for core in range(2):
            total = chip_sums(got_ref, core)
            for at in range(core, peers, 2):
                out_ref[at] = total


def spread(two, got):
    rows, width = two.shape[1:]
    peers, held, lanes = got.shape
    steps = width // lanes
    return pl.pallas_call(
        spread_kernel,
        grid=(steps + 1,),
        in_specs=[
            pl.BlockSpec((2, rows, lanes), lambda i: (0, 0, jnp.minimum(i, steps - 1))),
            pl.BlockSpec((peers, rows, lanes), lambda i: (0, held // rows - 1, 0)),
        ],
        out_specs=pl.BlockSpec((peers, rows, lanes), lambda i: (0, 0, i)),
        out_shape=pltpu.HBM((peers, rows, width + lanes), BF),
        compiler_params=params(8, "arbitrary"),
        name="spread",
    )(two, in_hbm(got))


def exchange(x):
    return lax.all_to_all(x, AXES, 0, 0, tiled=True)


def core_pairs():
    return [(i, i ^ 1) for i in range(lax.axis_size("dom"))]


def chip_grads(left, right, grad):
    first_core = lax.axis_index("dom") % 2 == 0
    theirs = tn(jnp.where(first_core, right, left), grad).astype(BF)
    arrived = lax.ppermute(theirs, "dom", core_pairs())
    ours = tn(jnp.where(first_core, left, right), grad)
    return (ours + arrived.astype(F32)).astype(BF)


def local(
    table, accum, w_self1, w_nbr1, w_self2, w_nbr2,
    fetch_owner, fetch_row, self_slot, nbr_one, nbr_two, cotangent,
):
    devices = lax.axis_size("grp") * lax.axis_size("dom")
    count = fetch_row.shape[0]
    emb = table.shape[1]
    nodes = self_slot.shape[0]
    cap = max(2, 2 * count // devices)
    slots = devices * cap
    ring_up = [(i, (i + 1) % devices) for i in range(devices)]
    ring_down = [(j, i) for i, j in ring_up]
    slot_row = self_slot.reshape(1, nodes)

    pos, wanted = prep(fetch_owner.reshape(1, count), fetch_row.reshape(1, count), devices, cap)
    incoming = exchange(wanted)
    mid_t, mid, edge_t, edge = counts(nbr_two.T, (nodes, 2 * BORDER), BORDER)
    found = pick(incoming, table)
    replies = exchange(found.reshape(devices, cap, emb))
    adj_t, adj = counts(nbr_one.T, (count,), 0)
    inc_row = incoming.reshape(1, slots)

    selfs, pooled_one, before_one, hidden = layer_one(
        pos, slot_row, replies.reshape(slots, emb), adj, w_self1, w_nbr1
    )
    before = lax.ppermute(hidden[nodes - BORDER :], AXES, ring_up)
    after = lax.ppermute(hidden[:BORDER], AXES, ring_down)
    own = nn(hidden, w_self2)
    pool = nn(mid, hidden)
    embedded, pooled_two, grad_two, grad_pool, grad_edge = layer_two(
        own, pool, edge, edge_t, after, before, w_nbr2, cotangent
    )
    to_first = lax.ppermute(grad_edge[:BORDER], AXES, ring_up)
    to_last = lax.ppermute(grad_edge[BORDER:], AXES, ring_down)
    chip_two = chip_grads(hidden, pooled_two, grad_two)
    hid = chip_two.shape[1]
    parts_two = exchange(chip_two.reshape(devices, -1, hid))
    grad_hidden = nt(grad_two, w_self2) + nn(mid_t, grad_pool)
    grad_one, grad_slots = back_one(
        grad_hidden, to_first, to_last, before_one, slot_row, adj_t, w_self1, w_nbr1, pos, slots
    )
    chip_one = chip_grads(selfs, pooled_one, grad_one)
    down, across = chip_one.shape[0] // 8, chip_one.shape[1] // emb
    tiles = chip_one.reshape(down, 8, across, emb).transpose(2, 0, 1, 3)
    sent = jnp.concatenate(
        [grad_slots.reshape(devices, cap, emb), tiles.reshape(devices, 8, emb)], axis=1
    )
    got = exchange(sent)
    mine = exchange(spread(two_sum(parts_two), got))
    new_table, new_accum = update(inc_row, got, table, accum)
    other = lax.ppermute(mine, "dom", core_pairs())
    first_core = lax.axis_index("dom") % 2 == 0

    def of_one(x):
        x = x[:, :, hid:].reshape(across, down, 8, emb).transpose(1, 2, 0, 3)
        return x.reshape(chip_one.shape)

    def of_two(x):
        return x[:, :, :hid].reshape(chip_two.shape)

    grads = []
    for of in (of_one, of_two):
        grads.append(of(jnp.where(first_core, mine, other)))
        grads.append(of(jnp.where(first_core, other, mine)))
    return (embedded, new_table, new_accum) + tuple(grads)


def solution(mesh):
    rows = P(AXES, None)
    flat = P(AXES)
    in_specs = (rows, flat, P(), P(), P(), P(), rows, flat, flat, rows, rows, rows)
    out_specs = (rows, rows, flat, P(), P(), P(), P())
    return jax.shard_map(
        local, mesh=mesh, in_specs=in_specs, out_specs=out_specs, check_vma=False
    )
```

```python
import jax
import jax.numpy as jnp
from jax import lax
from jax.experimental import pallas as pl
from jax.experimental.pallas import tpu as pltpu
from jax.sharding import PartitionSpec as P


BORDER = 64
AXES = ("grp", "dom")
epsilon = 1e-06
learning_rate = 0.1
BF = jnp.bfloat16
F32 = jnp.float32
I32 = jnp.int32
I16 = jnp.int16
MIB = 1024 * 1024


def iota(shape, dim):
    return lax.broadcasted_iota(I32, shape, dim)


def nn(a, b):
    return lax.dot_general(a, b, (((1,), (0,)), ((), ())), preferred_element_type=F32)


def nt(a, b):
    return lax.dot_general(a, b, (((1,), (1,)), ((), ())), preferred_element_type=F32)


def tn(a, b):
    return lax.dot_general(a, b, (((0,), (0,)), ((), ())), preferred_element_type=F32)


def hot(mask):
    return jnp.where(mask, 1.0, 0.0).astype(BF)


def hot_lanes(col, width):
    lanes = col.shape[1]
    index = iota(col.shape, 1).astype(I16)
    parts = []
    for at in range(0, width, lanes):
        hit = col == index + jnp.full(col.shape, at, I16)
        parts.append(jnp.where(hit, jnp.ones(col.shape, BF), jnp.zeros(col.shape, BF)))
    return jnp.concatenate(parts, axis=1)


def hot_rows(row, rows, first):
    shape = (rows, row.shape[1])
    index = iota(shape, 0).astype(I16)
    wanted = jnp.broadcast_to(row - first, shape).astype(I16)
    return jnp.where(index == wanted, jnp.ones(shape, BF), jnp.zeros(shape, BF))


def to_lanes(row):
    return jnp.broadcast_to(row, (128, row.shape[1])).T.astype(I16)


def logistic(v):
    return 1.0 / (1.0 + jnp.exp(-v))


def params(mib, *semantics):
    return pltpu.CompilerParams(
        dimension_semantics=semantics if semantics else None, vmem_limit_bytes=mib * MIB
    )


def in_hbm(x):
    return pltpu.with_memory_space_constraint(x, pltpu.HBM)


def cost(flops):
    return pl.CostEstimate(flops=flops, bytes_accessed=4 << 20, transcendentals=0)


def prep_kernel(owner_ref, row_ref, pos_ref, wanted_ref):
    count = owner_ref.shape[1]
    devices, cap = wanted_ref.shape
    owner = owner_ref[...]
    row = row_ref[...]
    owner_hot = hot(iota((devices, count), 0) == owner)
    earlier = hot(iota((count, count), 0) < iota((count, count), 1))
    before = nn(owner_hot, earlier)
    rank = jnp.sum(before * owner_hot.astype(F32), axis=0, keepdims=True).astype(I32)
    pos_ref[...] = owner * cap + rank
    at_rank = iota((cap, count), 0) == rank
    high = jnp.where(at_rank, (row >> 6).astype(F32), 0.0).astype(BF)
    low = jnp.where(at_rank, (row & 63).astype(F32), 0.0).astype(BF)
    wanted_ref[...] = (nt(owner_hot, high) * 64.0 + nt(owner_hot, low)).astype(I32)


def prep(owner, row, devices, cap):
    count = owner.shape[1]
    return pl.pallas_call(
        prep_kernel,
        out_shape=(
            jax.ShapeDtypeStruct((1, count), I32),
            jax.ShapeDtypeStruct((devices, cap), I32),
        ),
        compiler_params=params(8),
        name="prep",
    )(in_hbm(owner), in_hbm(row))


def counts_kernel(shift, width, nbr_ref, *out_refs):
    fanout, lanes = nbr_ref.shape
    base = 0
    lists = []
    for k in range(fanout):
        row = nbr_ref[k : k + 1, :]
        if shift:
            row = row - shift
            row = jnp.where(row < 0, row + width, row)
        lists.append(jnp.broadcast_to(row, (16, lanes)).astype(I16))
    index = iota((16, lanes), 0).astype(I16)
    unit = jnp.full((16, lanes), 1.0 / fanout, BF)
    none = jnp.zeros((16, lanes), BF)
    for adj_t_ref, adj_ref in zip(out_refs[::2], out_refs[1::2]):
        for first in range(0, adj_t_ref.shape[0], 128):
            rows = []
            for r in range(first, first + 128, 16):
                at = index + jnp.full((16, lanes), base + r, I16)
                acc = none
                for k in range(fanout):
                    acc = acc + jnp.where(lists[k] == at, unit, none)
                rows.append(acc)
            block = jnp.concatenate(rows, axis=0)
            adj_t_ref[first : first + 128, :] = block
            adj_ref[:, first : first + 128] = block.T
        base += adj_t_ref.shape[0]


def counts(nbr_t, widths, shift):
    fanout, nodes = nbr_t.shape
    block = 128
    specs, shapes = [], []
    for width in widths:
        specs += [
            pl.BlockSpec((width, block), lambda i: (0, i)),
            pl.BlockSpec((block, width), lambda i: (i, 0)),
        ]
        shapes += [pltpu.HBM((width, nodes), BF), pltpu.HBM((nodes, width), BF)]
    return pl.pallas_call(
        lambda *refs: counts_kernel(shift, sum(widths), *refs),
        grid=(nodes // block,),
        in_specs=[pl.BlockSpec((fanout, block), lambda i: (0, i))],
        out_specs=specs,
        out_shape=shapes,
        compiler_params=params(8, "arbitrary"),
        cost_estimate=cost(4 << 30),
    )(nbr_t)


def pick_kernel(inc_ref, table_ref, out_ref, col_ref, acc_ref, turn_ref):
    i = pl.program_id(0)
    peers, cap = inc_ref.shape
    rows, width = table_ref.shape

    @pl.when(i == 0)
    def _():
        for c in range(cap):
            col_ref[c * peers : (c + 1) * peers, :] = jnp.broadcast_to(
                inc_ref[:, c : c + 1], (peers, 128)
            ).astype(I16)
        acc_ref[...] = jnp.zeros(acc_ref.shape, F32)

    chunk = table_ref[...].astype(BF)
    base = (jnp.zeros((512, 128), I32) + i * rows).astype(I16)

    for at in range(0, acc_ref.shape[0], 512):
        at = pl.ds(at, 512)
        acc_ref[at, :] += nn(hot_lanes(col_ref[at, :] - base, rows), chunk)

    @pl.when(i == pl.num_programs(0) - 1)
    def _():
        for c in range(cap):
            for h in range(width // 128):
                turn_ref.at[h][pl.ds(c, peers, stride=cap), :] = acc_ref[
                    c * peers : (c + 1) * peers, h * 128 : (h + 1) * 128
                ]
        for h in range(width // 128):
            out_ref[:, h * 128 : (h + 1) * 128] = turn_ref[h].astype(BF)


def pick(incoming, table):
    devices, cap = incoming.shape
    rows, width = table.shape
    slots = devices * cap
    block = 1024
    return pl.pallas_call(
        pick_kernel,
        grid=(rows // block,),
        in_specs=[
            pl.BlockSpec((devices, cap), lambda i: (0, 0)),
            pl.BlockSpec((block, width), lambda i: (i, 0)),
        ],
        out_specs=pl.BlockSpec((slots, width), lambda i: (0, 0)),
        out_shape=pltpu.HBM((slots, width), BF),
        scratch_shapes=[
            pltpu.VMEM((slots, 128), I16),
            pltpu.VMEM((slots, width), F32),
            pltpu.VMEM((width // 128, slots, 128), F32),
        ],
        compiler_params=params(24, "arbitrary"),
        name="pick",
    )(incoming, in_hbm(table))


def nodes_of_one(slot_row, adj, fetched_ref, ws_ref, wn_ref):
    self_hot = hot_lanes(to_lanes(slot_row), fetched_ref.shape[0])
    selfs = nn(self_hot, fetched_ref[...]).astype(BF)
    pooled = nn(adj, fetched_ref[...]).astype(BF)
    before = nn(selfs, ws_ref[...]) + nn(pooled, wn_ref[...])
    return selfs, pooled, before, (before * logistic(before)).astype(BF)


def border_kernel(
    pos_ref, slot_ref, replies_ref, head_ref, tail_ref, ws_ref, wn_ref,
    fetched_ref, head_out_ref, tail_out_ref,
):
    fetch = fetched_ref.shape[0]
    nodes = slot_ref.shape[1]
    for at in range(0, fetch, 512):
        place = hot_lanes(to_lanes(pos_ref[:, at : at + 512]), replies_ref.shape[0])
        fetched_ref[at : at + 512, :] = nn(place, replies_ref[...]).astype(BF)
    slots = jnp.concatenate([slot_ref[:, :BORDER], slot_ref[:, nodes - BORDER :]], axis=1)
    adj = jnp.concatenate([head_ref[...], tail_ref[...]], axis=0)
    hidden = nodes_of_one(slots, adj, fetched_ref, ws_ref, wn_ref)[3]
    head_out_ref[...] = hidden[:BORDER]
    tail_out_ref[...] = hidden[BORDER:]


def border(pos, slot, replies, adj, w_self, w_nbr):
    nodes, fetch = adj.shape
    slots = replies.shape[0]
    emb, hid = w_self.shape
    whole = lambda i: (0, 0)
    return pl.pallas_call(
        border_kernel,
        grid=(1,),
        in_specs=[
            pl.BlockSpec((1, fetch), whole),
            pl.BlockSpec((1, nodes), whole),
            pl.BlockSpec((slots, emb), whole),
            pl.BlockSpec((BORDER, fetch), whole),
            pl.BlockSpec((BORDER, fetch), lambda i: (nodes // BORDER - 1, 0)),
            pl.BlockSpec((emb, hid), whole),
            pl.BlockSpec((emb, hid), whole),
        ],
        out_specs=[
            pl.BlockSpec((fetch, emb), whole),
            pl.BlockSpec((BORDER, hid), whole),
            pl.BlockSpec((BORDER, hid), whole),
        ],
        out_shape=(
            jax.ShapeDtypeStruct((fetch, emb), BF),
            jax.ShapeDtypeStruct((BORDER, hid), BF),
            jax.ShapeDtypeStruct((BORDER, hid), BF),
        ),
        compiler_params=params(24, "arbitrary"),
        name="border",
    )(pos, slot, replies, in_hbm(adj), in_hbm(adj), in_hbm(w_self), in_hbm(w_nbr))


def layer_one_kernel(
    slot_ref, fetched_ref, adj_ref, ws_ref, wn_ref, selfs_ref, pooled_ref, before_ref, hidden_ref
):
    selfs, pooled, before, hidden = nodes_of_one(
        slot_ref[...], adj_ref[...], fetched_ref, ws_ref, wn_ref
    )
    selfs_ref[...] = selfs
    pooled_ref[...] = pooled
    before_ref[...] = before
    hidden_ref[...] = hidden


def layer_one(slot, fetched, adj, w_self, w_nbr):
    nodes, fetch = adj.shape
    emb, hid = w_self.shape
    block = 256
    rows = lambda i: (i, 0)
    whole = lambda i: (0, 0)
    return pl.pallas_call(
        layer_one_kernel,
        grid=(nodes // block,),
        in_specs=[
            pl.BlockSpec((1, block), lambda i: (0, i)),
            pl.BlockSpec((fetch, emb), whole),
            pl.BlockSpec((block, fetch), rows),
            pl.BlockSpec((emb, hid), whole),
            pl.BlockSpec((emb, hid), whole),
        ],
        out_specs=[
            pl.BlockSpec((block, emb), rows),
            pl.BlockSpec((block, emb), rows),
            pl.BlockSpec((block, hid), rows),
            pl.BlockSpec((block, hid), rows),
        ],
        out_shape=(
            pltpu.HBM((nodes, emb), BF),
            pltpu.HBM((nodes, emb), BF),
            pltpu.HBM((nodes, hid), F32),
            jax.ShapeDtypeStruct((nodes, hid), BF),
        ),
        compiler_params=params(20, "arbitrary"),
        cost_estimate=cost(2 << 30),
        name="layer_one",
    )(slot, fetched, in_hbm(adj), in_hbm(w_self), in_hbm(w_nbr))


def layer_two_kernel(
    own_ref, pool_ref, edge_ref, edge_t_ref, after_ref, before_in_ref, wn_ref, up_ref,
    emb_ref, pooled_ref, grad_ref, gpool_ref, gedge_ref,
):
    block = own_ref.shape[0]

    @pl.when(pl.program_id(0) == 0)
    def _():
        gedge_ref[...] = jnp.zeros(gedge_ref.shape, F32)

    halo = jnp.concatenate([after_ref[...], before_in_ref[...]], axis=0)
    half = 256
    for at in range(0, block, half):
        rows = pl.ds(at, half)
        pooled = (pool_ref[rows, :] + nn(edge_ref[rows, :], halo)).astype(BF)
        pooled_ref[rows, :] = pooled
        before = own_ref[rows, :] + nn(pooled, wn_ref[...])
        gate = logistic(before)
        lifted = before * gate
        scale = lax.rsqrt(jnp.mean(lifted * lifted, axis=1, keepdims=True) + epsilon)
        normed = lifted * scale
        emb_ref[rows, :] = normed.astype(BF)
        up = up_ref[rows, :]
        grad_lifted = scale * (up - normed * jnp.mean(up * normed, axis=1, keepdims=True))
        grad = (grad_lifted * (gate + lifted * (1.0 - gate))).astype(BF)
        grad_ref[rows, :] = grad
        gpool = nt(grad, wn_ref[...]).astype(BF)
        gpool_ref[rows, :] = gpool
        gedge_ref[...] += nn(edge_t_ref[:, rows], gpool)


def layer_two(own, pool, edge, edge_t, after, before, w_nbr, upstream):
    nodes, hid = own.shape
    block = 256
    rows = lambda i: (i, 0)
    whole = lambda i: (0, 0)
    return pl.pallas_call(
        layer_two_kernel,
        grid=(nodes // block,),
        in_specs=[
            pl.BlockSpec((block, hid), rows),
            pl.BlockSpec((block, hid), rows),
            pl.BlockSpec((block, 2 * BORDER), rows),
            pl.BlockSpec((2 * BORDER, block), lambda i: (0, i)),
            pl.BlockSpec((BORDER, hid), whole),
            pl.BlockSpec((BORDER, hid), whole),
            pl.BlockSpec((hid, hid), whole),
            pl.BlockSpec((block, hid), rows),
        ],
        out_specs=[
            pl.BlockSpec((block, hid), rows),
            pl.BlockSpec((block, hid), rows),
            pl.BlockSpec((block, hid), rows),
            pl.BlockSpec((block, hid), rows),
            pl.BlockSpec((2 * BORDER, hid), whole),
        ],
        out_shape=(
            jax.ShapeDtypeStruct((nodes, hid), BF),
            jax.ShapeDtypeStruct((nodes, hid), BF),
            jax.ShapeDtypeStruct((nodes, hid), BF),
            jax.ShapeDtypeStruct((nodes, hid), BF),
            jax.ShapeDtypeStruct((2 * BORDER, hid), F32),
        ),
        compiler_params=params(28, "arbitrary"),
        name="layer_two",
    )(own, pool, edge, edge_t, after, before, w_nbr, upstream)


def back_one_kernel(
    gh_ref, first_ref, last_ref, before_ref, slot_ref, adj_t_ref, ws_ref, wn_ref, pos_ref,
    grad_ref, out_ref, gh_scr, acc_ref,
):
    i = pl.program_id(0)
    last = pl.num_programs(0) - 1
    block = gh_ref.shape[0]
    fetch = acc_ref.shape[0]
    gh_scr[...] = gh_ref[...]

    @pl.when(i == 0)
    def _():
        gh_scr[0:BORDER, :] += first_ref[...]
        acc_ref[...] = jnp.zeros(acc_ref.shape, F32)

    @pl.when(i == last)
    def _():
        gh_scr[block - BORDER : block, :] += last_ref[...]

    before = before_ref[...]
    gate = logistic(before)
    grad = (gh_scr[...] * (gate + before * gate * (1.0 - gate))).astype(BF)
    grad_ref[...] = grad
    gself = nt(grad, ws_ref[...])
    high = gself.astype(BF)
    low = (gself - high.astype(F32)).astype(BF)
    gpool = nt(grad, wn_ref[...]).astype(BF)
    self_t = hot_rows(slot_ref[...], fetch, 0)
    acc_ref[...] += nn(self_t, high) + nn(self_t, low) + nn(adj_t_ref[...], gpool)

    @pl.when(i == last)
    def _():
        total = acc_ref[...].astype(BF)
        pos = pos_ref[...]
        slots = out_ref.shape[0]
        for at in range(0, slots, 256):
            place_t = hot_rows(pos, 256, at)
            out_ref[at : at + 256, :] = nn(place_t, total).astype(BF)


def back_one(gh, first, last, before, slot, adj_t, w_self, w_nbr, pos, slots):
    nodes, hid = gh.shape
    emb = w_self.shape[0]
    fetch = adj_t.shape[0]
    block = 256
    rows = lambda i: (i, 0)
    cols = lambda i: (0, i)
    whole = lambda i: (0, 0)
    return pl.pallas_call(
        back_one_kernel,
        grid=(nodes // block,),
        in_specs=[
            pl.BlockSpec((block, hid), rows),
            pl.BlockSpec((BORDER, hid), whole),
            pl.BlockSpec((BORDER, hid), whole),
            pl.BlockSpec((block, hid), rows),
            pl.BlockSpec((1, block), cols),
            pl.BlockSpec((fetch, block), cols),
            pl.BlockSpec((emb, hid), whole),
            pl.BlockSpec((emb, hid), whole),
            pl.BlockSpec((1, fetch), whole),
        ],
        out_specs=[
            pl.BlockSpec((block, hid), rows),
            pl.BlockSpec((slots, emb), whole),
        ],
        out_shape=(
            pltpu.HBM((nodes, hid), BF),
            pltpu.HBM((slots, emb), BF),
        ),
        scratch_shapes=[pltpu.VMEM((block, hid), F32), pltpu.VMEM((fetch, emb), F32)],
        compiler_params=params(24, "arbitrary"),
        name="back_one",
    )(
        gh, first, last, in_hbm(before), slot, in_hbm(adj_t), in_hbm(w_self), in_hbm(w_nbr), pos,
    )


def update_kernel(
    inc_ref, got_ref, table_ref, accum_ref, new_table_ref, new_accum_ref, returned_ref
):
    i = pl.program_id(0)
    block, width = table_ref.shape
    slots = returned_ref.shape[0]
    peers = got_ref.shape[0]

    @pl.when(i == 0)
    def _():
        returned_ref[...] = got_ref[:, : slots // peers, :].reshape(slots, width)

    inc = inc_ref[...]
    step = 512
    grads = jnp.zeros((block, width), F32)
    for at in range(0, slots, step):
        rows_hot = hot_rows(inc[:, at : at + step], block, i * block)
        grads = grads + nn(rows_hot, returned_ref[at : at + step, :])
    square = jnp.mean(grads * grads, axis=1, keepdims=True)
    accum = accum_ref[0]
    new_accum_ref[0] = accum + jnp.broadcast_to(square, (block, 128)).T[0:1, :]
    total = jnp.broadcast_to(accum, (128, block)).T + square
    factor = learning_rate / (jnp.sqrt(total) + epsilon)
    for at in range(0, width, 128):
        new_table_ref[:, at : at + 128] = (
            table_ref[:, at : at + 128] - grads[:, at : at + 128] * factor
        )


def update(inc_row, got, table, accum):
    rows, width = table.shape
    slots = inc_row.shape[1]
    block = 512
    shaped = accum.reshape(rows // block, 1, block)
    new_table, new_accum = pl.pallas_call(
        update_kernel,
        grid=(rows // block,),
        in_specs=[
            pl.BlockSpec((1, slots), lambda i: (0, 0)),
            pl.BlockSpec(got.shape, lambda i: (0, 0, 0)),
            pl.BlockSpec((block, width), lambda i: (i, 0)),
            pl.BlockSpec((1, 1, block), lambda i: (i, 0, 0)),
        ],
        out_specs=[
            pl.BlockSpec((block, width), lambda i: (i, 0)),
            pl.BlockSpec((1, 1, block), lambda i: (i, 0, 0)),
        ],
        out_shape=(
            jax.ShapeDtypeStruct((rows, width), F32),
            jax.ShapeDtypeStruct(shaped.shape, F32),
        ),
        scratch_shapes=[pltpu.VMEM((slots, width), BF)],
        compiler_params=params(16, "arbitrary"),
        cost_estimate=cost(4 << 30),
        name="update",
    )(inc_row, in_hbm(got), in_hbm(table), shaped)
    return new_table, new_accum.reshape(rows)


def chip_sums(parts_ref, core):
    total = parts_ref[core].astype(F32)
    for at in range(core + 2, parts_ref.shape[0], 2):
        total = total + parts_ref[at].astype(F32)
    return total.astype(BF)


def two_sum_kernel(parts_ref, out_ref):
    for core in range(2):
        out_ref[core] = chip_sums(parts_ref, core)


def two_sum(parts):
    peers, rows, width = parts.shape
    lanes = 512
    return pl.pallas_call(
        two_sum_kernel,
        grid=(width // lanes,),
        in_specs=[pl.BlockSpec((peers, rows, lanes), lambda i: (0, 0, i))],
        out_specs=pl.BlockSpec((2, rows, lanes), lambda i: (0, 0, i)),
        out_shape=jax.ShapeDtypeStruct((2, rows, width), BF),
        compiler_params=params(8, "arbitrary"),
        cost_estimate=cost(1 << 30),
        name="two_sum",
    )(in_hbm(parts))


def spread_two_kernel(two_ref, out_ref):
    for core in range(2):
        for at in range(core, out_ref.shape[0], 2):
            out_ref[at] = two_ref[core]


def spread_one_kernel(got_ref, rest_ref, out_ref):
    for core in range(2):
        total = chip_sums(got_ref, core)
        for at in range(core, out_ref.shape[0], 2):
            out_ref[at] = total


def spread_two(two, peers, lanes):
    rows, width = two.shape[1:]
    return pl.pallas_call(
        spread_two_kernel,
        grid=(width // lanes,),
        in_specs=[pl.BlockSpec((2, rows, lanes), lambda i: (0, 0, i))],
        out_specs=pl.BlockSpec((peers, rows, lanes), lambda i: (0, 0, i)),
        out_shape=pltpu.HBM((peers, rows, width + lanes), BF),
        compiler_params=params(8, "arbitrary"),
        cost_estimate=cost(1 << 30),
        name="spread_two",
    )(two)


def spread_one(got, rest):
    peers, held, lanes = got.shape
    rows, width = rest.shape[1:]
    return pl.pallas_call(
        spread_one_kernel,
        grid=(1,),
        in_specs=[
            pl.BlockSpec((peers, rows, lanes), lambda i: (0, held // rows - 1, 0)),
            pl.BlockSpec(memory_space=pl.ANY),
        ],
        out_specs=pl.BlockSpec((peers, rows, lanes), lambda i: (0, 0, width // lanes - 1)),
        out_shape=pltpu.HBM(rest.shape, BF),
        input_output_aliases={1: 0},
        compiler_params=params(8, "arbitrary"),
        name="spread_one",
    )(in_hbm(got), rest)


SETTLE_CHUNKS = 4


def settle_kernel(which_ref, mine_ref, *refs):
    outs, buffer_ref, sem_in, sem_out = refs[-7:-3], refs[-3], refs[-2], refs[-1]
    lanes = outs[2].shape[2]
    peers, _, total = buffer_ref.shape
    width = total - lanes
    part = peers // SETTLE_CHUNKS

    def fetch(q):
        rows = pl.ds(q * part, part)
        return pltpu.make_async_copy(mine_ref.at[rows], buffer_ref.at[rows], sem_in.at[q])

    for q in range(SETTLE_CHUNKS):
        fetch(q).start()
    for core in range(2):

        @pl.when(which_ref[0] == core)
        def _():
            one_ref, two_ref = outs[core], outs[2 + core]
            moves = []
            for q in range(SETTLE_CHUNKS):
                fetch(q).wait()
                rows = pl.ds(q * part, part)
                moves.append(
                    pltpu.make_async_copy(
                        buffer_ref.at[rows, :, pl.ds(0, lanes)], two_ref.at[rows], sem_out.at[q, 0]
                    )
                )
                moves.append(
                    pltpu.make_async_copy(
                        buffer_ref.at[rows, :, pl.ds(lanes, width)],
                        one_ref.at[:, :, pl.ds(q * width, width)],
                        sem_out.at[q, 1],
                    )
                )
                moves[-2].start()
                moves[-1].start()
            for move in moves:
                move.wait()


def settle(which, mine, before):
    peers, rows, total = mine.shape
    lanes = 1024
    width = total - lanes
    assert lanes // width == SETTLE_CHUNKS
    one = pltpu.HBM((peers // SETTLE_CHUNKS, rows, lanes), BF)
    two = pltpu.HBM((peers, rows, lanes), BF)
    hbm = pl.BlockSpec(memory_space=pl.ANY)
    return pl.pallas_call(
        settle_kernel,
        in_specs=[pl.BlockSpec(memory_space=pltpu.SMEM), hbm] + [hbm] * len(before),
        out_specs=[hbm] * 4,
        out_shape=[one, one, two, two],
        input_output_aliases={2 + k: k for k in range(len(before))},
        scratch_shapes=[
            pltpu.VMEM(mine.shape, BF),
            pltpu.SemaphoreType.DMA((SETTLE_CHUNKS,)),
            pltpu.SemaphoreType.DMA((SETTLE_CHUNKS, 2)),
        ],
        compiler_params=params(8),
    )(which, in_hbm(mine), *before)


def exchange(x):
    return lax.all_to_all(x, AXES, 0, 0, tiled=True)


def core_pairs():
    return [(i, i ^ 1) for i in range(lax.axis_size("dom"))]


def chip_grads(left, right, grad):
    first_core = lax.axis_index("dom") % 2 == 0
    theirs = tn(jnp.where(first_core, right, left), grad).astype(BF)
    arrived = lax.ppermute(theirs, "dom", core_pairs())
    ours = lax.optimization_barrier(tn(jnp.where(first_core, left, right), grad))
    return (ours + arrived.astype(F32)).astype(BF)


def local(
    table, accum, w_self1, w_nbr1, w_self2, w_nbr2,
    fetch_owner, fetch_row, self_slot, nbr_one, nbr_two, cotangent,
):
    devices = lax.axis_size("grp") * lax.axis_size("dom")
    count = fetch_row.shape[0]
    emb = table.shape[1]
    nodes = self_slot.shape[0]
    cap = max(2, 2 * count // devices)
    slots = devices * cap
    ring_up = [(i, (i + 1) % devices) for i in range(devices)]
    ring_down = [(j, i) for i, j in ring_up]
    slot_row = self_slot.reshape(1, nodes)

    pos, wanted = prep(fetch_owner.reshape(1, count), fetch_row.reshape(1, count), devices, cap)
    incoming = exchange(wanted)
    mid_t, mid, edge_t, edge = counts(nbr_two.T, (nodes, 2 * BORDER), BORDER)
    found = pick(incoming, table)
    replies = exchange(found.reshape(devices, cap, emb))
    adj_t, adj = counts(nbr_one.T, (count,), 0)
    inc_row = incoming.reshape(1, slots)

    fetched, head, tail = border(
        pos, slot_row, replies.reshape(slots, emb), adj, w_self1, w_nbr1
    )
    before = lax.ppermute(tail, AXES, ring_up)
    after = lax.ppermute(head, AXES, ring_down)
    selfs, pooled_one, before_one, hidden = layer_one(slot_row, fetched, adj, w_self1, w_nbr1)
    own = nn(hidden, w_self2)
    pool = nn(mid, hidden)
    embedded, pooled_two, grad_two, grad_pool, grad_edge = layer_two(
        own, pool, edge, edge_t, after, before, w_nbr2, cotangent
    )
    to_first = lax.ppermute(grad_edge[:BORDER], AXES, ring_up)
    to_last = lax.ppermute(grad_edge[BORDER:], AXES, ring_down)
    chip_two = chip_grads(hidden, pooled_two, grad_two)
    hid = chip_two.shape[1]
    parts_two = exchange(chip_two.reshape(devices, -1, hid))
    grad_hidden = nt(grad_two, w_self2) + nn(mid_t, grad_pool)
    grad_one, grad_slots = back_one(
        grad_hidden, to_first, to_last, before_one, slot_row, adj_t, w_self1, w_nbr1, pos, slots
    )
    chip_one = chip_grads(selfs, pooled_one, grad_one)
    down, across = chip_one.shape[0] // 8, chip_one.shape[1] // emb
    tiles = chip_one.reshape(down, 8, across, emb).transpose(2, 0, 1, 3)
    sent = jnp.concatenate(
        [grad_slots.reshape(devices, cap, emb), tiles.reshape(devices, 8, emb)], axis=1
    )
    got = exchange(sent)
    rest = spread_two(two_sum(parts_two), devices, emb)
    mine = exchange(spread_one(got, rest))
    new_table, new_accum = update(inc_row, got, table, accum)
    other = lax.ppermute(mine, "dom", core_pairs())
    core = lax.axis_index("dom") % 2
    grads = settle(core.reshape(1), mine, ())
    grads = settle((1 - core).reshape(1), other, grads)
    shapes = (chip_one.shape, chip_one.shape, chip_two.shape, chip_two.shape)
    grads = tuple(g.reshape(shape) for g, shape in zip(grads, shapes))
    return (embedded, new_table, new_accum) + grads


def solution(mesh):
    rows = P(AXES, None)
    flat = P(AXES)
    in_specs = (rows, flat, P(), P(), P(), P(), rows, flat, flat, rows, rows, rows)
    out_specs = (rows, rows, flat, P(), P(), P(), P())
    return jax.shard_map(
        local, mesh=mesh, in_specs=in_specs, out_specs=out_specs, check_vma=False
    )
```

```python
import jax
import jax.numpy as jnp
from jax import lax
from jax.experimental import pallas as pl
from jax.experimental.pallas import tpu as pltpu
from jax.sharding import PartitionSpec as P


BORDER = 64
AXES = ("grp", "dom")
epsilon = 1e-06
learning_rate = 0.1
BF = jnp.bfloat16
F32 = jnp.float32
I32 = jnp.int32
I16 = jnp.int16
MIB = 1024 * 1024


def iota(shape, dim):
    return lax.broadcasted_iota(I32, shape, dim)


def nn(a, b):
    return lax.dot_general(a, b, (((1,), (0,)), ((), ())), preferred_element_type=F32)


def nt(a, b):
    return lax.dot_general(a, b, (((1,), (1,)), ((), ())), preferred_element_type=F32)


def tn(a, b):
    return lax.dot_general(a, b, (((0,), (0,)), ((), ())), preferred_element_type=F32)


def hot(mask):
    return jnp.where(mask, 1.0, 0.0).astype(BF)


def hot_lanes(col, width):
    lanes = col.shape[1]
    index = iota(col.shape, 1).astype(I16)
    parts = []
    for at in range(0, width, lanes):
        hit = col == index + jnp.full(col.shape, at, I16)
        parts.append(jnp.where(hit, jnp.ones(col.shape, BF), jnp.zeros(col.shape, BF)))
    return jnp.concatenate(parts, axis=1)


def hot_rows(row, rows, first):
    shape = (rows, row.shape[1])
    index = iota(shape, 0).astype(I16)
    wanted = jnp.broadcast_to(row - first, shape).astype(I16)
    return jnp.where(index == wanted, jnp.ones(shape, BF), jnp.zeros(shape, BF))


def to_lanes(row):
    return jnp.broadcast_to(row, (128, row.shape[1])).T.astype(I16)


def logistic(v):
    return 1.0 / (1.0 + jnp.exp(-v))


def params(mib, *semantics):
    return pltpu.CompilerParams(
        dimension_semantics=semantics if semantics else None, vmem_limit_bytes=mib * MIB
    )


def in_hbm(x):
    return pltpu.with_memory_space_constraint(x, pltpu.HBM)


def cost(flops):
    return pl.CostEstimate(flops=flops, bytes_accessed=4 << 20, transcendentals=0)


def prep_kernel(owner_ref, row_ref, pos_ref, wanted_ref):
    count = owner_ref.shape[1]
    devices, cap = wanted_ref.shape
    owner = owner_ref[...]
    row = row_ref[...]
    owner_hot = hot(iota((devices, count), 0) == owner)
    earlier = hot(iota((count, count), 0) < iota((count, count), 1))
    before = nn(owner_hot, earlier)
    rank = jnp.sum(before * owner_hot.astype(F32), axis=0, keepdims=True).astype(I32)
    pos_ref[...] = owner * cap + rank
    at_rank = iota((cap, count), 0) == rank
    high = jnp.where(at_rank, (row >> 6).astype(F32), 0.0).astype(BF)
    low = jnp.where(at_rank, (row & 63).astype(F32), 0.0).astype(BF)
    wanted_ref[...] = (nt(owner_hot, high) * 64.0 + nt(owner_hot, low)).astype(I32)


def prep(owner, row, devices, cap):
    count = owner.shape[1]
    return pl.pallas_call(
        prep_kernel,
        out_shape=(
            jax.ShapeDtypeStruct((1, count), I32),
            jax.ShapeDtypeStruct((devices, cap), I32),
        ),
        compiler_params=params(8),
        name="prep",
    )(in_hbm(owner), in_hbm(row))


def counts_kernel(shift, width, nbr_ref, *out_refs):
    fanout, lanes = nbr_ref.shape
    base = 0
    lists = []
    for k in range(fanout):
        row = nbr_ref[k : k + 1, :]
        if shift:
            row = row - shift
            row = jnp.where(row < 0, row + width, row)
        lists.append(jnp.broadcast_to(row, (16, lanes)).astype(I16))
    index = iota((16, lanes), 0).astype(I16)
    unit = jnp.full((16, lanes), 1.0 / fanout, BF)
    none = jnp.zeros((16, lanes), BF)
    for adj_t_ref, adj_ref in zip(out_refs[::2], out_refs[1::2]):
        for first in range(0, adj_t_ref.shape[0], 128):
            rows = []
            for r in range(first, first + 128, 16):
                at = index + jnp.full((16, lanes), base + r, I16)
                acc = none
                for k in range(fanout):
                    acc = acc + jnp.where(lists[k] == at, unit, none)
                rows.append(acc)
            block = jnp.concatenate(rows, axis=0)
            adj_t_ref[first : first + 128, :] = block
            adj_ref[:, first : first + 128] = block.T
        base += adj_t_ref.shape[0]


def counts(nbr_t, widths, shift):
    fanout, nodes = nbr_t.shape
    block = 128
    specs, shapes = [], []
    for width in widths:
        specs += [
            pl.BlockSpec((width, block), lambda i: (0, i)),
            pl.BlockSpec((block, width), lambda i: (i, 0)),
        ]
        shapes += [pltpu.HBM((width, nodes), BF), pltpu.HBM((nodes, width), BF)]
    return pl.pallas_call(
        lambda *refs: counts_kernel(shift, sum(widths), *refs),
        grid=(nodes // block,),
        in_specs=[pl.BlockSpec((fanout, block), lambda i: (0, i))],
        out_specs=specs,
        out_shape=shapes,
        compiler_params=params(8, "arbitrary"),
        cost_estimate=cost(4 << 30),
    )(nbr_t)


def pick_kernel(inc_ref, table_ref, out_ref, col_ref, acc_ref, wide_ref):
    i = pl.program_id(0)
    peers, cap = inc_ref.shape
    rows, _ = table_ref.shape

    @pl.when(i == 0)
    def _():
        for c in range(cap):
            wide_ref[pl.ds(c, peers, stride=cap), :] = jnp.broadcast_to(
                inc_ref[:, c : c + 1], (peers, 128)
            )
        col_ref[...] = wide_ref[...].astype(I16)
        acc_ref[...] = jnp.zeros(acc_ref.shape, F32)

    chunk = table_ref[...].astype(BF)
    base = (jnp.zeros((512, 128), I32) + i * rows).astype(I16)

    for at in range(0, acc_ref.shape[0], 512):
        at = pl.ds(at, 512)
        acc_ref[at, :] += nn(hot_lanes(col_ref[at, :] - base, rows), chunk)

    @pl.when(i == pl.num_programs(0) - 1)
    def _():
        out_ref[...] = acc_ref[...].astype(BF)


def pick(incoming, table):
    devices, cap = incoming.shape
    rows, width = table.shape
    slots = devices * cap
    block = 1024
    return pl.pallas_call(
        pick_kernel,
        grid=(rows // block,),
        in_specs=[
            pl.BlockSpec((devices, cap), lambda i: (0, 0)),
            pl.BlockSpec((block, width), lambda i: (i, 0)),
        ],
        out_specs=pl.BlockSpec((slots, width), lambda i: (0, 0)),
        out_shape=pltpu.HBM((slots, width), BF),
        scratch_shapes=[
            pltpu.VMEM((slots, 128), I16),
            pltpu.VMEM((slots, width), F32),
            pltpu.VMEM((slots, 128), I32),
        ],
        compiler_params=params(24, "arbitrary"),
        name="pick",
    )(incoming, in_hbm(table))


def nodes_of_one(slot_row, adj, fetched_ref, ws_ref, wn_ref):
    self_hot = hot_lanes(to_lanes(slot_row), fetched_ref.shape[0])
    selfs = nn(self_hot, fetched_ref[...]).astype(BF)
    pooled = nn(adj, fetched_ref[...]).astype(BF)
    before = nn(selfs, ws_ref[...]) + nn(pooled, wn_ref[...])
    return selfs, pooled, before, (before * logistic(before)).astype(BF)


def border_kernel(
    pos_ref, slot_ref, replies_ref, head_ref, tail_ref, ws_ref, wn_ref,
    fetched_ref, head_out_ref, tail_out_ref,
):
    fetch = fetched_ref.shape[0]
    nodes = slot_ref.shape[1]
    for at in range(0, fetch, 512):
        place = hot_lanes(to_lanes(pos_ref[:, at : at + 512]), replies_ref.shape[0])
        fetched_ref[at : at + 512, :] = nn(place, replies_ref[...]).astype(BF)
    slots = jnp.concatenate([slot_ref[:, :BORDER], slot_ref[:, nodes - BORDER :]], axis=1)
    adj = jnp.concatenate([head_ref[...], tail_ref[...]], axis=0)
    hidden = nodes_of_one(slots, adj, fetched_ref, ws_ref, wn_ref)[3]
    head_out_ref[...] = hidden[:BORDER]
    tail_out_ref[...] = hidden[BORDER:]


def border(pos, slot, replies, adj, w_self, w_nbr):
    nodes, fetch = adj.shape
    slots = replies.shape[0]
    emb, hid = w_self.shape
    whole = lambda i: (0, 0)
    return pl.pallas_call(
        border_kernel,
        grid=(1,),
        in_specs=[
            pl.BlockSpec((1, fetch), whole),
            pl.BlockSpec((1, nodes), whole),
            pl.BlockSpec((slots, emb), whole),
            pl.BlockSpec((BORDER, fetch), whole),
            pl.BlockSpec((BORDER, fetch), lambda i: (nodes // BORDER - 1, 0)),
            pl.BlockSpec((emb, hid), whole),
            pl.BlockSpec((emb, hid), whole),
        ],
        out_specs=[
            pl.BlockSpec((fetch, emb), whole),
            pl.BlockSpec((BORDER, hid), whole),
            pl.BlockSpec((BORDER, hid), whole),
        ],
        out_shape=(
            jax.ShapeDtypeStruct((fetch, emb), BF),
            jax.ShapeDtypeStruct((BORDER, hid), BF),
            jax.ShapeDtypeStruct((BORDER, hid), BF),
        ),
        compiler_params=params(24, "arbitrary"),
        name="border",
    )(pos, slot, replies, in_hbm(adj), in_hbm(adj), in_hbm(w_self), in_hbm(w_nbr))


def layer_one_kernel(
    slot_ref, fetched_ref, adj_ref, ws_ref, wn_ref, selfs_ref, pooled_ref, before_ref, hidden_ref
):
    selfs, pooled, before, hidden = nodes_of_one(
        slot_ref[...], adj_ref[...], fetched_ref, ws_ref, wn_ref
    )
    selfs_ref[...] = selfs
    pooled_ref[...] = pooled
    before_ref[...] = before
    hidden_ref[...] = hidden


def layer_one(slot, fetched, adj, w_self, w_nbr):
    nodes, fetch = adj.shape
    emb, hid = w_self.shape
    block = 512
    rows = lambda i: (i, 0)
    whole = lambda i: (0, 0)
    return pl.pallas_call(
        layer_one_kernel,
        grid=(nodes // block,),
        in_specs=[
            pl.BlockSpec((1, block), lambda i: (0, i)),
            pl.BlockSpec((fetch, emb), whole),
            pl.BlockSpec((block, fetch), rows),
            pl.BlockSpec((emb, hid), whole),
            pl.BlockSpec((emb, hid), whole),
        ],
        out_specs=[
            pl.BlockSpec((block, emb), rows),
            pl.BlockSpec((block, emb), rows),
            pl.BlockSpec((block, hid), rows),
            pl.BlockSpec((block, hid), rows),
        ],
        out_shape=(
            pltpu.HBM((nodes, emb), BF),
            pltpu.HBM((nodes, emb), BF),
            pltpu.HBM((nodes, hid), F32),
            jax.ShapeDtypeStruct((nodes, hid), BF),
        ),
        compiler_params=params(28, "arbitrary"),
        cost_estimate=cost(2 << 30),
        name="layer_one",
    )(slot, fetched, in_hbm(adj), in_hbm(w_self), in_hbm(w_nbr))


def layer_two_kernel(
    own_ref, pool_ref, edge_ref, edge_t_ref, after_ref, before_in_ref, wn_ref, up_ref,
    emb_ref, pooled_ref, grad_ref, gpool_ref, gedge_ref,
):
    block = own_ref.shape[0]

    @pl.when(pl.program_id(0) == 0)
    def _():
        gedge_ref[...] = jnp.zeros(gedge_ref.shape, F32)

    halo = jnp.concatenate([after_ref[...], before_in_ref[...]], axis=0)
    half = 256
    for at in range(0, block, half):
        rows = pl.ds(at, half)
        pooled = (pool_ref[rows, :] + nn(edge_ref[rows, :], halo)).astype(BF)
        pooled_ref[rows, :] = pooled
        before = own_ref[rows, :] + nn(pooled, wn_ref[...])
        gate = logistic(before)
        lifted = before * gate
        scale = lax.rsqrt(jnp.mean(lifted * lifted, axis=1, keepdims=True) + epsilon)
        normed = lifted * scale
        emb_ref[rows, :] = normed.astype(BF)
        up = up_ref[rows, :]
        grad_lifted = scale * (up - normed * jnp.mean(up * normed, axis=1, keepdims=True))
        grad = (grad_lifted * (gate + lifted * (1.0 - gate))).astype(BF)
        grad_ref[rows, :] = grad
        gpool = nt(grad, wn_ref[...]).astype(BF)
        gpool_ref[rows, :] = gpool
        gedge_ref[...] += nn(edge_t_ref[:, rows], gpool)


def layer_two(own, pool, edge, edge_t, after, before, w_nbr, upstream):
    nodes, hid = own.shape
    block = 256
    rows = lambda i: (i, 0)
    whole = lambda i: (0, 0)
    return pl.pallas_call(
        layer_two_kernel,
        grid=(nodes // block,),
        in_specs=[
            pl.BlockSpec((block, hid), rows),
            pl.BlockSpec((block, hid), rows),
            pl.BlockSpec((block, 2 * BORDER), rows),
            pl.BlockSpec((2 * BORDER, block), lambda i: (0, i)),
            pl.BlockSpec((BORDER, hid), whole),
            pl.BlockSpec((BORDER, hid), whole),
            pl.BlockSpec((hid, hid), whole),
            pl.BlockSpec((block, hid), rows),
        ],
        out_specs=[
            pl.BlockSpec((block, hid), rows),
            pl.BlockSpec((block, hid), rows),
            pl.BlockSpec((block, hid), rows),
            pl.BlockSpec((block, hid), rows),
            pl.BlockSpec((2 * BORDER, hid), whole),
        ],
        out_shape=(
            jax.ShapeDtypeStruct((nodes, hid), BF),
            jax.ShapeDtypeStruct((nodes, hid), BF),
            jax.ShapeDtypeStruct((nodes, hid), BF),
            jax.ShapeDtypeStruct((nodes, hid), BF),
            jax.ShapeDtypeStruct((2 * BORDER, hid), F32),
        ),
        compiler_params=params(28, "arbitrary"),
        name="layer_two",
    )(own, pool, edge, edge_t, after, before, w_nbr, upstream)


def back_one_kernel(
    gh_ref, first_ref, last_ref, before_ref, slot_ref, adj_t_ref, ws_ref, wn_ref, pos_ref,
    grad_ref, out_ref, gh_scr, acc_ref,
):
    i = pl.program_id(0)
    last = pl.num_programs(0) - 1
    block = gh_ref.shape[0]
    fetch = acc_ref.shape[0]
    gh_scr[...] = gh_ref[...]

    @pl.when(i == 0)
    def _():
        gh_scr[0:BORDER, :] += first_ref[...]
        acc_ref[...] = jnp.zeros(acc_ref.shape, F32)

    @pl.when(i == last)
    def _():
        gh_scr[block - BORDER : block, :] += last_ref[...]

    before = before_ref[...]
    gate = logistic(before)
    grad = (gh_scr[...] * (gate + before * gate * (1.0 - gate))).astype(BF)
    grad_ref[...] = grad
    gself = nt(grad, ws_ref[...])
    high = gself.astype(BF)
    low = (gself - high.astype(F32)).astype(BF)
    gpool = nt(grad, wn_ref[...]).astype(BF)
    self_t = hot_rows(slot_ref[...], fetch, 0)
    acc_ref[...] += nn(self_t, high) + nn(self_t, low) + nn(adj_t_ref[...], gpool)

    @pl.when(i == last)
    def _():
        total = acc_ref[...].astype(BF)
        pos = pos_ref[...]
        slots = out_ref.shape[0]
        for at in range(0, slots, 256):
            place_t = hot_rows(pos, 256, at)
            out_ref[at : at + 256, :] = nn(place_t, total).astype(BF)


def back_one(gh, first, last, before, slot, adj_t, w_self, w_nbr, pos, slots):
    nodes, hid = gh.shape
    emb = w_self.shape[0]
    fetch = adj_t.shape[0]
    block = 256
    rows = lambda i: (i, 0)
    cols = lambda i: (0, i)
    whole = lambda i: (0, 0)
    return pl.pallas_call(
        back_one_kernel,
        grid=(nodes // block,),
        in_specs=[
            pl.BlockSpec((block, hid), rows),
            pl.BlockSpec((BORDER, hid), whole),
            pl.BlockSpec((BORDER, hid), whole),
            pl.BlockSpec((block, hid), rows),
            pl.BlockSpec((1, block), cols),
            pl.BlockSpec((fetch, block), cols),
            pl.BlockSpec((emb, hid), whole),
            pl.BlockSpec((emb, hid), whole),
            pl.BlockSpec((1, fetch), whole),
        ],
        out_specs=[
            pl.BlockSpec((block, hid), rows),
            pl.BlockSpec((slots, emb), whole),
        ],
        out_shape=(
            pltpu.HBM((nodes, hid), BF),
            pltpu.HBM((slots, emb), BF),
        ),
        scratch_shapes=[pltpu.VMEM((block, hid), F32), pltpu.VMEM((fetch, emb), F32)],
        compiler_params=params(24, "arbitrary"),
        name="back_one",
    )(
        gh, first, last, in_hbm(before), slot, in_hbm(adj_t), in_hbm(w_self), in_hbm(w_nbr), pos,
    )


def update_kernel(
    inc_ref, got_ref, table_ref, accum_ref, new_table_ref, new_accum_ref, returned_ref
):
    i = pl.program_id(0)
    block, width = table_ref.shape
    slots = returned_ref.shape[0]
    peers = got_ref.shape[0]

    @pl.when(i == 0)
    def _():
        returned_ref[...] = got_ref[:, : slots // peers, :].reshape(slots, width)

    inc = inc_ref[...]
    step = 512
    grads = jnp.zeros((block, width), F32)
    for at in range(0, slots, step):
        rows_hot = hot_rows(inc[:, at : at + step], block, i * block)
        grads = grads + nn(rows_hot, returned_ref[at : at + step, :])
    square = jnp.mean(grads * grads, axis=1, keepdims=True)
    accum = accum_ref[0]
    new_accum_ref[0] = accum + jnp.broadcast_to(square, (block, 128)).T[0:1, :]
    total = jnp.broadcast_to(accum, (128, block)).T + square
    factor = learning_rate / (jnp.sqrt(total) + epsilon)
    for at in range(0, width, 128):
        new_table_ref[:, at : at + 128] = (
            table_ref[:, at : at + 128] - grads[:, at : at + 128] * factor
        )


def update(inc_row, got, table, accum):
    rows, width = table.shape
    slots = inc_row.shape[1]
    block = 512
    shaped = accum.reshape(rows // block, 1, block)
    new_table, new_accum = pl.pallas_call(
        update_kernel,
        grid=(rows // block,),
        in_specs=[
            pl.BlockSpec((1, slots), lambda i: (0, 0)),
            pl.BlockSpec(got.shape, lambda i: (0, 0, 0)),
            pl.BlockSpec((block, width), lambda i: (i, 0)),
            pl.BlockSpec((1, 1, block), lambda i: (i, 0, 0)),
        ],
        out_specs=[
            pl.BlockSpec((block, width), lambda i: (i, 0)),
            pl.BlockSpec((1, 1, block), lambda i: (i, 0, 0)),
        ],
        out_shape=(
            jax.ShapeDtypeStruct((rows, width), F32),
            jax.ShapeDtypeStruct(shaped.shape, F32),
        ),
        scratch_shapes=[pltpu.VMEM((slots, width), BF)],
        compiler_params=params(16, "arbitrary"),
        cost_estimate=cost(4 << 30),
        name="update",
    )(inc_row, in_hbm(got), in_hbm(table), shaped)
    return new_table, new_accum.reshape(rows)


def chip_sums(parts_ref, core):
    total = parts_ref[core].astype(F32)
    for at in range(core + 2, parts_ref.shape[0], 2):
        total = total + parts_ref[at].astype(F32)
    return total.astype(BF)


def two_sum_kernel(parts_ref, out_ref):
    for core in range(2):
        out_ref[core] = chip_sums(parts_ref, core)


def two_sum(parts):
    peers, rows, width = parts.shape
    lanes = 512
    return pl.pallas_call(
        two_sum_kernel,
        grid=(width // lanes,),
        in_specs=[pl.BlockSpec((peers, rows, lanes), lambda i: (0, 0, i))],
        out_specs=pl.BlockSpec((2, rows, lanes), lambda i: (0, 0, i)),
        out_shape=jax.ShapeDtypeStruct((2, rows, width), BF),
        compiler_params=params(8, "arbitrary"),
        cost_estimate=cost(1 << 30),
        name="two_sum",
    )(in_hbm(parts))


def spread_two_kernel(two_ref, out_ref):
    for core in range(2):
        for at in range(core, out_ref.shape[0], 2):
            out_ref[at] = two_ref[core]


def spread_one_kernel(got_ref, rest_ref, out_ref):
    for core in range(2):
        total = chip_sums(got_ref, core)
        for at in range(core, out_ref.shape[0], 2):
            out_ref[at] = total


def spread_two(two, peers, lanes):
    rows, width = two.shape[1:]
    return pl.pallas_call(
        spread_two_kernel,
        grid=(width // lanes,),
        in_specs=[pl.BlockSpec((2, rows, lanes), lambda i: (0, 0, i))],
        out_specs=pl.BlockSpec((peers, rows, lanes), lambda i: (0, 0, i)),
        out_shape=pltpu.HBM((peers, rows, width + lanes), BF),
        compiler_params=params(8, "arbitrary"),
        cost_estimate=cost(1 << 30),
        name="spread_two",
    )(two)


def spread_one(got, rest):
    peers, held, lanes = got.shape
    rows, width = rest.shape[1:]
    return pl.pallas_call(
        spread_one_kernel,
        grid=(lanes // 128,),
        in_specs=[
            pl.BlockSpec((peers, rows, 128), lambda i: (0, held // rows - 1, i)),
            pl.BlockSpec(memory_space=pl.ANY),
        ],
        out_specs=pl.BlockSpec((peers, rows, 128), lambda i: (0, 0, (width - lanes) // 128 + i)),
        out_shape=pltpu.HBM(rest.shape, BF),
        input_output_aliases={1: 0},
        compiler_params=params(8, "arbitrary"),
        name="spread_one",
    )(in_hbm(got), rest)


SETTLE_CHUNKS = 4


def settle_kernel(which_ref, mine_ref, *refs):
    outs, buffer_ref, sem_in, sem_out = refs[-7:-3], refs[-3], refs[-2], refs[-1]
    lanes = outs[2].shape[2]
    peers, _, total = buffer_ref.shape
    width = total - lanes
    part = peers // SETTLE_CHUNKS

    def fetch(q):
        rows = pl.ds(q * part, part)
        return pltpu.make_async_copy(mine_ref.at[rows], buffer_ref.at[rows], sem_in.at[q])

    for q in range(SETTLE_CHUNKS):
        fetch(q).start()
    for core in range(2):

        @pl.when(which_ref[0] == core)
        def _():
            one_ref, two_ref = outs[core], outs[2 + core]
            moves = []
            for q in range(SETTLE_CHUNKS):
                fetch(q).wait()
                rows = pl.ds(q * part, part)
                moves.append(
                    pltpu.make_async_copy(
                        buffer_ref.at[rows, :, pl.ds(0, lanes)], two_ref.at[rows], sem_out.at[q, 0]
                    )
                )
                moves.append(
                    pltpu.make_async_copy(
                        buffer_ref.at[rows, :, pl.ds(lanes, width)],
                        one_ref.at[:, :, pl.ds(q * width, width)],
                        sem_out.at[q, 1],
                    )
                )
                moves[-2].start()
                moves[-1].start()
            for move in moves:
                move.wait()


def settle(which, mine, before):
    peers, rows, total = mine.shape
    lanes = 1024
    width = total - lanes
    assert lanes // width == SETTLE_CHUNKS
    one = pltpu.HBM((peers // SETTLE_CHUNKS, rows, lanes), BF)
    two = pltpu.HBM((peers, rows, lanes), BF)
    hbm = pl.BlockSpec(memory_space=pl.ANY)
    return pl.pallas_call(
        settle_kernel,
        in_specs=[pl.BlockSpec(memory_space=pltpu.SMEM), hbm] + [hbm] * len(before),
        out_specs=[hbm] * 4,
        out_shape=[one, one, two, two],
        input_output_aliases={2 + k: k for k in range(len(before))},
        scratch_shapes=[
            pltpu.VMEM(mine.shape, BF),
            pltpu.SemaphoreType.DMA((SETTLE_CHUNKS,)),
            pltpu.SemaphoreType.DMA((SETTLE_CHUNKS, 2)),
        ],
        compiler_params=params(8),
    )(which, in_hbm(mine), *before)


def exchange(x):
    return lax.all_to_all(x, AXES, 0, 0, tiled=True)


def core_pairs():
    return [(i, i ^ 1) for i in range(lax.axis_size("dom"))]


def chip_grads(left, right, grad):
    first_core = lax.axis_index("dom") % 2 == 0
    theirs = tn(jnp.where(first_core, right, left), grad).astype(BF)
    arrived = lax.ppermute(theirs, "dom", core_pairs())
    ours = lax.optimization_barrier(tn(jnp.where(first_core, left, right), grad))
    return (ours + arrived.astype(F32)).astype(BF)


def local(
    table, accum, w_self1, w_nbr1, w_self2, w_nbr2,
    fetch_owner, fetch_row, self_slot, nbr_one, nbr_two, cotangent,
):
    devices = lax.axis_size("grp") * lax.axis_size("dom")
    count = fetch_row.shape[0]
    emb = table.shape[1]
    nodes = self_slot.shape[0]
    cap = max(2, 2 * count // devices)
    slots = devices * cap
    ring_up = [(i, (i + 1) % devices) for i in range(devices)]
    ring_down = [(j, i) for i, j in ring_up]
    slot_row = self_slot.reshape(1, nodes)

    pos, wanted = prep(fetch_owner.reshape(1, count), fetch_row.reshape(1, count), devices, cap)
    incoming = exchange(wanted)
    mid_t, mid, edge_t, edge = counts(nbr_two.T, (nodes, 2 * BORDER), BORDER)
    found = pick(incoming, table)
    replies = exchange(found.reshape(devices, cap, emb))
    adj_t, adj = counts(nbr_one.T, (count,), 0)
    inc_row = incoming.reshape(1, slots)

    fetched, head, tail = border(
        pos, slot_row, replies.reshape(slots, emb), adj, w_self1, w_nbr1
    )
    before = lax.ppermute(tail, AXES, ring_up)
    after = lax.ppermute(head, AXES, ring_down)
    selfs, pooled_one, before_one, hidden = layer_one(slot_row, fetched, adj, w_self1, w_nbr1)
    own = nn(hidden, w_self2)
    pool = nn(mid, hidden)
    embedded, pooled_two, grad_two, grad_pool, grad_edge = layer_two(
        own, pool, edge, edge_t, after, before, w_nbr2, cotangent
    )
    to_first = lax.ppermute(grad_edge[:BORDER], AXES, ring_up)
    to_last = lax.ppermute(grad_edge[BORDER:], AXES, ring_down)
    chip_two = chip_grads(hidden, pooled_two, grad_two)
    hid = chip_two.shape[1]
    parts_two = exchange(chip_two.reshape(devices, -1, hid))
    grad_hidden = nt(grad_two, w_self2) + nn(mid_t, grad_pool)
    grad_one, grad_slots = back_one(
        grad_hidden, to_first, to_last, before_one, slot_row, adj_t, w_self1, w_nbr1, pos, slots
    )
    chip_one = chip_grads(selfs, pooled_one, grad_one)
    down, across = chip_one.shape[0] // 8, chip_one.shape[1] // emb
    tiles = chip_one.reshape(down, 8, across, emb).transpose(2, 0, 1, 3)
    sent = jnp.concatenate(
        [grad_slots.reshape(devices, cap, emb), tiles.reshape(devices, 8, emb)], axis=1
    )
    got = exchange(sent)
    rest = spread_two(two_sum(parts_two), devices, emb)
    mine = exchange(spread_one(got, rest))
    new_table, new_accum = update(inc_row, got, table, accum)
    other = lax.ppermute(mine, "dom", core_pairs())
    core = lax.axis_index("dom") % 2
    grads = settle(core.reshape(1), mine, ())
    grads = settle((1 - core).reshape(1), other, grads)
    shapes = (chip_one.shape, chip_one.shape, chip_two.shape, chip_two.shape)
    grads = tuple(g.reshape(shape) for g, shape in zip(grads, shapes))
    return (embedded, new_table, new_accum) + grads


def solution(mesh):
    rows = P(AXES, None)
    flat = P(AXES)
    in_specs = (rows, flat, P(), P(), P(), P(), rows, flat, flat, rows, rows, rows)
    out_specs = (rows, rows, flat, P(), P(), P(), P())
    return jax.shard_map(
        local, mesh=mesh, in_specs=in_specs, out_specs=out_specs, check_vma=False
    )
```
